32 devices in a mesh: batch: 4 (over y, x), heads: 8 (over z, core).
Axes of the slice: x: 2, y: 2, z: 4, core: 2. Of those that a mesh axis runs over, the one named last changes fastest.
Arguments:
- draft_ids: int32 [192, 8], P('batch'), may hold values from 0 to 50279
- accepted: int32 [192], P('batch'), may hold values from 1 to 8
- embedding: bfloat16 [50280, 2560], P(None, 'heads'), may hold values from -6 to 6
- norm_gain: float32 [2, 2560], replicated, may hold values from 0.5 to 1.5
- w_zx: bfloat16 [2, 2560, 8, 128], P(None, None, 'heads'), may hold values from -0.125 to 0.125
- w_dt: bfloat16 [2, 2560, 8], P(None, None, 'heads'), may hold values from -0.125 to 0.125
- w_bc: bfloat16 [2, 2560, 256], P(None, None, 'heads'), may hold values from -0.125 to 0.125
- dt_bias: float32 [2, 8], P(None, 'heads'), may hold values from -4 to -1
- decay_rate: float32 [2, 8], P(None, 'heads'), may hold values from 1 to 16
- skip_weight: float32 [2, 8], P(None, 'heads'), may hold values from 0.5 to 1.5
- conv_x_w: bfloat16 [2, 4, 512], P(None, None, 'heads'), may hold values from -3 to 3
- conv_x_b: bfloat16 [2, 512], P(None, 'heads'), may hold values from -3 to 3
- conv_bc_w: bfloat16 [2, 4, 256], P(None, None, 'heads'), may hold values from -3 to 3
- conv_bc_b: bfloat16 [2, 256], P(None, 'heads'), may hold values from -3 to 3
- gate_gain: float32 [2, 512], P(None, 'heads'), may hold values from 0.5 to 1.5
- out_w: bfloat16 [2, 512, 2560], P(None, 'heads'), may hold values from -0.375 to 0.375
- ssm_state: float32 [2, 192, 8, 64, 128], P(None, 'batch', 'heads'), may hold values from -1.6 to 1.6
- conv_x_state: bfloat16 [2, 192, 3, 512], P(None, 'batch', None, 'heads'), may hold values from -6 to 6
- conv_bc_state: bfloat16 [2, 192, 3, 256], P(None, 'batch', None, 'heads'), may hold values from -6 to 6
Outputs:
- hidden_out: bfloat16 [1536, 2560], P('batch', 'heads')
- new_ssm: float32 [2, 192, 8, 64, 128], P(None, 'batch', 'heads')
- new_conv_x: bfloat16 [2, 192, 3, 512], P(None, 'batch', None, 'heads')
- new_conv_bc: bfloat16 [2, 192, 3, 256], P(None, 'batch', None, 'heads')
The draws below stay inside these ranges and needn't reach their ends.
Inputs may be any that keep to these rules, and one draw needn't show every extreme that they name: `accepted`: the number of a sequence's draft tokens that are kept, counted from the first.
All inputs are finite; a program needn't handle non-finite values.
Results may differ from the reference program's by a relative error of at most 0.015.
Values may be sent and summed in bfloat16 or wider, within the bound.
A program may use at most 128 MiB of HBM per device.

```python
import math
import jax
import jax.numpy as jnp
import numpy as np
from jax import lax

D = 2560
P_SIZE = 64
N = 128
VOCAB = 50280
KCONV = 4
DRAFT = 8
LAYERS = 2
HEADS = 8
INNER = 512
SEQS = 192


def set_ends(drawn, own_key, least, top_value):
    dims = drawn.shape
    index_at = [jax.random.randint(jax.random.fold_in(own_key, axis), (), 0, dims[axis]) for axis in range(len(dims))]
    drawn = drawn.at[tuple(index_at)].set(least)
    longest = dims.index(max(dims))
    index_at[longest] = (index_at[longest] + 1) % dims[longest]
    return drawn.at[tuple(index_at)].set(top_value)


def strengthened(values, key, source, target, shards_of, factor):
    owner, partner = [(jnp.arange(values.shape[position]) // (values.shape[position] // shards_of)).reshape([-1 if axis == position else 1 for axis in range(values.ndim)]) for position in (source, target)]
    chosen = jax.random.permutation(key, shards_of)[partner]
    strong = (owner == chosen) | (owner == (partner + shards_of // 2) % shards_of)
    return jnp.where(strong, factor * values, values)


def shard_levels(own_key, dims, split, low, largest):
    def one(axis_at, parts):
        heights = jax.random.uniform(jax.random.fold_in(jax.random.fold_in(own_key, 6), axis_at), (parts,), jnp.float32, low / len(split), largest / len(split))
        return jnp.repeat(jnp.exp(heights), dims[axis_at] // parts).reshape((-1,) + (1,) * (len(dims) - axis_at - 1))

    gain = one(*split[0])
    for cut in split[1:]:
        gain = gain * one(*cut)
    return gain


def rank_table(number_of, lean):
    loads = [(1 << 20) // math.isqrt(grade ** lean) + 1 for grade in range(1, number_of + 1)]
    scale = 1 + sum(loads) // (1 << 30)
    return np.cumsum(np.array([max(1, weight // scale) for weight in loads]))


def ranked_ids(stream_key, dims, amount, slope):
    listing = rank_table(amount, slope)
    ticket = jax.random.randint(jax.random.fold_in(stream_key, 1), dims, 0, int(listing[amount - 1]))
    grade = jnp.searchsorted(jnp.asarray(listing, jnp.int32), ticket, side="right")
    return jax.random.permutation(jax.random.fold_in(stream_key, 2), amount)[grade].astype(jnp.int32)


def centred(rng, dims, scale, bound, cuts=(), kind=jnp.bfloat16):
    result = scale * jax.random.normal(rng, dims, jnp.float32)
    if cuts:
        result = result * shard_levels(rng, dims, cuts, -0.22, 0.18)
    return jnp.clip(result, -bound, bound).astype(kind)


def bell_draw_with(key, shape, scale, bound, cuts, heavy, kind=jnp.bfloat16):
    array = scale * jax.random.normal(key, shape, jnp.float32)
    if cuts:
        array = array * shard_levels(key, shape, cuts, -0.22, 0.18)
    return jnp.clip(strengthened(array, jax.random.fold_in(key, 3), *heavy), -bound, bound).astype(kind)


def setup_inputs(seed: int = 0) -> dict:
    seeds = jax.random.split(jax.random.key(seed), 20)
    return {
        "draft_ids": set_ends(ranked_ids(seeds[0], (SEQS, DRAFT), VOCAB, 2), jax.random.fold_in(seeds[0], 3), 0, VOCAB - 1).astype(jnp.int32),
        "accepted": set_ends(jax.random.randint(seeds[1], (SEQS,), 1, DRAFT + 1), jax.random.fold_in(seeds[1], 1), 1, DRAFT).astype(jnp.int32),
        "embedding": centred(seeds[2], (VOCAB, D), 1.0, 6.0, ((1, 8),)),
        "norm_gain": jnp.clip(1.0 + 0.1 * jax.random.normal(seeds[3], (LAYERS, D), jnp.float32), 0.5, 1.5),
        "w_zx": centred(seeds[4], (LAYERS, D, HEADS, 2 * P_SIZE), D ** -0.5, 0.125, ((2, 8),)),
        "w_dt": centred(seeds[5], (LAYERS, D, HEADS), D ** -0.5, 0.125, ((2, 8),)),
        "w_bc": centred(seeds[6], (LAYERS, D, 2 * N), D ** -0.5, 0.125, ((2, 8),)),
        "dt_bias": jnp.clip(-4.0 + 3.0 * jax.random.uniform(seeds[7], (LAYERS, HEADS), jnp.float32) ** shard_levels(seeds[7], (LAYERS, HEADS), ((1, 8),), -0.2, 0.2), -4.0, -1.0),
        "decay_rate": jnp.clip(jnp.exp(math.log(16.0) - 2.7725887 * jax.random.uniform(seeds[8], (LAYERS, HEADS), jnp.float32) ** shard_levels(seeds[8], (LAYERS, HEADS), ((1, 8),), -0.2, 0.2)), 1.0, 16.0),
        "skip_weight": jnp.clip(0.5 + 1.0 * jax.random.uniform(seeds[9], (LAYERS, HEADS), jnp.float32) ** shard_levels(seeds[9], (LAYERS, HEADS), ((1, 8),), -0.2, 0.2), 0.5, 1.5),
        "conv_x_w": centred(seeds[10], (LAYERS, KCONV, INNER), 0.5, 3.0, ((2, 8),)),
        "conv_x_b": centred(seeds[11], (LAYERS, INNER), 0.5, 3.0, ((1, 8),)),
        "conv_bc_w": centred(seeds[12], (LAYERS, KCONV, 2 * N), 0.5, 3.0, ((2, 8),)),
        "conv_bc_b": centred(seeds[13], (LAYERS, 2 * N), 0.5, 3.0, ((1, 8),)),
        "gate_gain": jnp.clip(1.0 + 0.1 * jax.random.normal(seeds[14], (LAYERS, INNER), jnp.float32), 0.5, 1.5),
        "out_w": bell_draw_with(seeds[15], (LAYERS, INNER, D), INNER ** -0.5, 0.375, ((1, 8),), (1, 2, 8, 2.0)),
        "ssm_state": centred(seeds[16], (LAYERS, SEQS, HEADS, P_SIZE, N), 0.2, 1.6, ((1, 4), (2, 8)), jnp.float32),
        "conv_x_state": centred(seeds[17], (LAYERS, SEQS, KCONV - 1, INNER), 1.0, 6.0, ((1, 4), (3, 8))),
        "conv_bc_state": centred(seeds[18], (LAYERS, SEQS, KCONV - 1, 2 * N), 1.0, 6.0, ((1, 4), (3, 8))),
    }


EPS = 1e-05

def rms_scale(total, count):
    return lax.rsqrt(total / count + EPS)

def convolve(window, weight, bias, count):
    weight = weight.astype(jnp.float32)
    acc = window[:, 0:count] * weight[0]
    for k in range(1, weight.shape[0]):
        acc = acc + window[:, k:k + count] * weight[k]
    return jax.nn.silu(acc + bias.astype(jnp.float32))

def keep_rows(window, accepted, kept_rows):
    last_start = window.shape[1] - kept_rows
    kept = window[:, 1:1 + kept_rows]
    for start in range(2, last_start + 1):
        kept = jnp.where((accepted == start)[:, None, None], window[:, start:start + kept_rows], kept)
    return kept

def recur(decay, step, values, bmat, cmat, skip, state, accepted):
    kept = state
    outputs = []
    for t in range(values.shape[1]):
        state = decay[:, t, None, None] * state + (step[:, t, None] * values[:, t])[:, :, None] * bmat[:, t, None, :]
        outputs.append(lax.optimization_barrier(jnp.sum(state * cmat[:, t, None, :], axis=-1)) + skip * values[:, t])
        kept = jnp.where((accepted == t + 1)[:, None, None], state, kept)
    return (jnp.stack(outputs, 1), kept)

def reference(draft_ids, accepted, embedding, norm_gain, w_zx, w_dt, w_bc, dt_bias, decay_rate, skip_weight, conv_x_w, conv_x_b, conv_bc_w, conv_bc_b, gate_gain, out_w, ssm_state, conv_x_state, conv_bc_state):
    seqs, draft = draft_ids.shape
    heads = w_zx.shape[2]
    width = w_zx.shape[3] // 2
    inner = heads * width
    model = embedding.shape[1]
    states = w_bc.shape[2] // 2
    kernel = conv_x_w.shape[1]
    stream = embedding[draft_ids.reshape(-1)]
    saved_state, saved_x, saved_bc = ([], [], [])
    for layer in range(LAYERS):
        value = stream.astype(jnp.float32)
        normed = (value * rms_scale(lax.optimization_barrier(jnp.sum(value * value, -1, keepdims=True)), model) * norm_gain[layer]).astype(jnp.bfloat16)
        zx = jnp.dot(normed, w_zx[layer].reshape(model, -1), preferred_element_type=jnp.float32).astype(jnp.bfloat16)
        zx = zx.reshape(seqs, draft, heads, 2, width)
        gate_z = zx[:, :, :, 0].astype(jnp.float32)
        values = zx[:, :, :, 1].reshape(seqs, draft, inner)
        dt_raw = jnp.dot(normed, w_dt[layer], preferred_element_type=jnp.float32).astype(jnp.bfloat16).reshape(seqs, draft, heads)
        bc = jnp.dot(normed, w_bc[layer], preferred_element_type=jnp.float32).astype(jnp.bfloat16).reshape(seqs, draft, 2 * states)
        window_x = jnp.concatenate([conv_x_state[layer], values], axis=1)
        xc = convolve(window_x.astype(jnp.float32), conv_x_w[layer], conv_x_b[layer], draft).reshape(seqs, draft, heads, width)
        window_bc = jnp.concatenate([conv_bc_state[layer], bc], axis=1)
        bcc = convolve(window_bc.astype(jnp.float32), conv_bc_w[layer], conv_bc_b[layer], draft).astype(jnp.bfloat16)
        bcc = lax.optimization_barrier(bcc).astype(jnp.float32)
        bmat = bcc[..., :states]
        cmat = bcc[..., states:]
        step = jax.nn.softplus(dt_raw.astype(jnp.float32) + dt_bias[layer])
        decay = jnp.exp(-step * decay_rate[layer])

        def run(pieces):
            return recur(pieces[0], pieces[1], pieces[2], bmat, cmat, pieces[3], pieces[4], accepted)
        outputs, kept = lax.map(run, (jnp.moveaxis(decay, 2, 0), jnp.moveaxis(step, 2, 0), jnp.moveaxis(xc, 2, 0), skip_weight[layer], jnp.moveaxis(ssm_state[layer], 1, 0)))
        outputs = jnp.moveaxis(outputs, 0, 2)
        saved_state.append(jnp.moveaxis(kept, 0, 1))
        saved_x.append(keep_rows(window_x, accepted, kernel - 1))
        saved_bc.append(keep_rows(window_bc, accepted, kernel - 1))
        gated = outputs * jax.nn.silu(gate_z)
        ssq = lax.optimization_barrier(jnp.sum(gated * gated, axis=(2, 3))).reshape(-1)
        u = (gated.reshape(seqs, draft, inner) * gate_gain[layer]).astype(jnp.bfloat16).reshape(-1, inner)
        mix = jnp.dot(u, out_w[layer], preferred_element_type=jnp.float32) * rms_scale(ssq, inner)[:, None]
        stream = (stream.astype(jnp.float32) + mix).astype(jnp.bfloat16)
    return (stream, jnp.stack(saved_state), jnp.stack(saved_x), jnp.stack(saved_bc))
```

```python
import functools

import jax
import jax.numpy as jnp
from jax import lax
from jax.experimental import pallas as pl
from jax.experimental.pallas import tpu as pltpu
from jax.sharding import PartitionSpec as P

LAYERS = 2
EPS = 1e-05
MESH = pl.DeviceIdType.MESH
LANES = 128
VMEM_LIMIT = 63 * 1024 * 1024
PROGRAM_LIMIT = 50 * 1024 * 1024
F32, BF16 = jnp.float32, jnp.bfloat16


def rms_scale(total, count):
    return lax.rsqrt(total / count + EPS)


def dot(a, b, ca=1, cb=0):
    return lax.dot_general(a, b, (((ca,), (cb,)), ((), ())), preferred_element_type=F32)


def round_up(x, m):
    return -(-x // m) * m


def silu(v):
    return v * (1.0 / (1.0 + jnp.exp(-v)))


def eye(n, dtype):
    row = lax.broadcasted_iota(jnp.int32, (n, n), 0)
    col = lax.broadcasted_iota(jnp.int32, (n, n), 1)
    return jnp.where(row == col, 1.0, 0.0).astype(dtype)


def remote(src, dst, send, recv, axis, device):
    return pltpu.make_async_remote_copy(
        src_ref=src, dst_ref=dst, send_sem=send, recv_sem=recv,
        device_id={axis: device}, device_id_type=MESH,
    )


class Place:
    def __init__(self, n, nb):
        self.n, self.nb, self.chips = n, nb, n // 2
        self.me = lax.axis_index("heads")
        self.b = lax.axis_index("batch")
        self.core = lax.rem(self.me, 2)
        self.chip = self.me // 2
        self.mate = self.me + 1 - 2 * self.core
        self.last = self.chips - 1

    def greet(self):
        barrier = pltpu.get_barrier_semaphore()
        for d in range(1, self.n):
            pl.semaphore_signal(
                barrier, inc=1, device_id={"heads": lax.rem(self.me + d, self.n)},
                device_id_type=MESH,
            )
        for k in range(1, self.nb):
            pl.semaphore_signal(
                barrier, inc=1, device_id={"batch": lax.rem(self.b + k, self.nb)},
                device_id_type=MESH,
            )
        pl.semaphore_wait(barrier, self.n + self.nb - 2)


class Line:
    def __init__(self, place, buf, sems, arrived):
        self.p, self.buf, self.sems, self.arrived = place, buf, sems, arrived

    def copy(self, kind, d, slot, device):
        ref = self.buf(slot)
        return remote(ref, ref, self.sems.at[kind, 0, d], self.sems.at[kind, 1, d], "heads", device)

    def start(self):
        p = self.p

        @pl.when(p.chip < p.last)
        def _():
            self.copy(0, 0, p.me, p.me + 2).start()

        @pl.when(p.chip > 0)
        def _():
            self.copy(1, 0, p.me, p.me - 2).start()

        self.arrived(0, p.me)

    def step(self, d):
        p = self.p

        @pl.when(p.chip >= d)
        def _():
            slot = p.me - 2 * d
            self.copy(0, d - 1, slot, slot).wait_recv()

            @pl.when(p.chip < p.last)
            def _():
                self.copy(0, d, slot, p.me + 2).start()

            self.arrived(d, slot)

        @pl.when(p.chip + d <= p.last)
        def _():
            slot = p.me + 2 * d
            self.copy(1, d - 1, slot, slot).wait_recv()

            @pl.when(p.chip > 0)
            def _():
                self.copy(1, d, slot, p.me - 2).start()

            self.arrived(p.last + d, slot)

    def each(self, fn):
        p = self.p
        fn(0, 0)
        for d in range(1, p.chips):
            @pl.when(p.chip >= d)
            def _(d=d):
                fn(d, -2 * d)

            @pl.when(p.chip + d <= p.last)
            def _(d=d):
                fn(p.last + d, 2 * d)

    def sent(self):
        p = self.p
        for d in range(p.chips - 1):
            @pl.when((p.chip >= d) & (p.chip < p.last))
            def _(d=d):
                self.copy(0, d, p.me, p.me).wait_send()

            @pl.when((p.chip + d <= p.last) & (p.chip > 0))
            def _(d=d):
                self.copy(1, d, p.me, p.me).wait_send()


class Direct:
    def __init__(self, place, out, sems):
        self.p, self.out, self.sems = place, out, sems

    def copy(self, slot, device, kind, c):
        ref = self.out.at[slot]
        return remote(ref, ref, self.sems.at[kind, 0, c], self.sems.at[kind, 1, c], "heads", device)

    def slot(self, c, core):
        p = self.p
        return 2 * lax.rem(p.chip + p.chips - c, p.chips) + core

    def order(self):
        return sorted(range(1, self.p.chips), key=lambda c: min(c, self.p.chips - c))

    def start(self):
        p = self.p
        self.copy(p.me, p.mate, 0, 0).start()
        for c in self.order():
            dst = 2 * lax.rem(p.chip + c, p.chips) + p.core
            self.copy(p.me, dst, 0, c).start()

    def relay(self):
        p = self.p
        for c in self.order():
            slot = self.slot(c, p.core)
            self.copy(slot, slot, 0, c).wait_recv()
            self.copy(slot, p.mate, 1, c).start()

    def finish(self):
        p = self.p
        self.copy(p.mate, p.mate, 0, 0).wait_recv()
        for c in range(1, p.chips):
            slot = self.slot(c, 1 - p.core)
            self.copy(slot, p.mate, 1, c).wait_recv()

    def sent(self):
        p = self.p
        for c in range(p.chips):
            self.copy(p.me, p.mate, 0, c).wait_send()
        for c in range(1, p.chips):
            self.copy(p.me, p.mate, 1, c).wait_send()


class Spread:
    def __init__(self, axis, me, n, src, dst, sems):
        self.axis, self.me, self.n = axis, me, n
        self.src, self.dst, self.sems = src, dst, sems

    def copy(self, d, peer, at):
        return remote(
            self.src(peer), self.dst(at), self.sems.at[0, d], self.sems.at[1, d], self.axis, peer
        )

    def start(self):
        for d in range(1, self.n):
            self.copy(d, lax.rem(self.me + d, self.n), self.me).start()

    def came(self):
        for d in range(1, self.n):
            peer = lax.rem(self.me + self.n - d, self.n)
            self.copy(d, peer, peer).wait_recv()

    def sent(self):
        for d in range(1, self.n):
            self.copy(d, lax.rem(self.me + d, self.n), self.me).wait_send()


def take_tokens(ids, table, tokens):
    draft, seqs = ids.shape
    rows = table.shape[0]
    lane = lax.broadcasted_iota(jnp.int32, (rows, LANES), 1)
    blocks = []
    for g in range(tokens // LANES):
        acc = jnp.zeros((rows, LANES), F32)
        at = g * LANES
        while at < (g + 1) * LANES:
            t, s0 = at // seqs, at % seqs
            count = min(seqs - s0, (g + 1) * LANES - at)
            unroll = 8
            while count % unroll:
                unroll //= 2

            def body(i, acc, t=t, s0=s0, j0=at - g * LANES, unroll=unroll):
                for k in range(unroll):
                    s = i * unroll + k
                    token = ids[t, s0 + s]
                    inside = token & (LANES - 1)
                    start = pl.multiple_of(token - inside, LANES)
                    block = table[:, pl.ds(start, LANES)].astype(F32)
                    shift = (j0 + s + LANES - inside) & (LANES - 1)
                    acc = jnp.where(lane == j0 + s, pltpu.roll(block, shift, 1), acc)
                return acc

            acc = lax.fori_loop(0, count // unroll, body, acc)
            at += count
        blocks.append(acc)
    return blocks


def split_rows(cols):
    if cols % 80:
        return [cols]
    return [cols * 2 // 5, cols * 2 // 5, cols // 5]


def lookup_kernel(cuts, vocab, *refs):
    ids, tail, table, part = refs[:4]
    tabs, sems = refs[4:-1], refs[-1]
    tokens = part.shape[1]
    full = vocab // LANES * LANES
    loads, first = [], 0
    for f, rows in enumerate(cuts):
        loads.append(
            pltpu.make_async_copy(
                table.at[pl.ds(first, rows), pl.ds(0, full)], tabs[f].at[:, pl.ds(0, full)],
                sems.at[f],
            )
        )
        loads[-1].start()
        first += rows
    first = 0
    for f, rows in enumerate(cuts):
        here = slice(first, first + rows)
        tabs[f][:, full:] = tail[here]
        loads[f].wait()
        for g, block in enumerate(take_tokens(ids, tabs[f], tokens)):
            part[here, g * LANES : (g + 1) * LANES] = block.astype(BF16)
        first += rows


def lookup(ids, table, tokens):
    cols, vocab = table.shape
    full = vocab // LANES * LANES
    cuts = split_rows(cols)
    return pl.pallas_call(
        functools.partial(lookup_kernel, cuts, vocab),
        grid=(1,),
        out_shape=jax.ShapeDtypeStruct((cols, tokens), BF16),
        in_specs=[
            pl.BlockSpec(memory_space=pltpu.SMEM),
            pl.BlockSpec((cols, LANES), lambda i: (0, full // LANES)),
            pl.BlockSpec(memory_space=pl.ANY),
        ],
        out_specs=pl.BlockSpec((cols, tokens), lambda i: (0, 0)),
        scratch_shapes=[pltpu.VMEM((rows, full + LANES), BF16) for rows in cuts]
        + [pltpu.SemaphoreType.DMA((len(cuts),))],
        compiler_params=pltpu.CompilerParams(vmem_limit_bytes=VMEM_LIMIT),
        name="lookup",
    )(ids, table, table)


def program_kernel(cfg, *refs):
    n, nb, blocks, draft = cfg
    (bias, rate_ref, skip_ref, accepted, gain, w_dt, x_w, x_b, bc_w, bc_b, gate_gain,
     x_state, bc_state, part, w_zx, w_bc, out_w, ssm,
     hidden, new_x, new_bc, h1) = refs[:22]
    refs = refs[22:]
    (stream, val, nrm, wl, gcol, wz, wb, ow, parts_src, parts, whole, bca, bcf, ua, sq, h0,
     c_s, b_s, x_s, y_s, k_s,
     load_sem, line_sems, w_line, w_batch, w_mate,
     mate_sems, bc_sems, u_sems, sq_sems, part_sems, part_batch) = refs
    p = Place(n, nb)
    me = p.me
    cols = part.shape[0]
    model = cols * n
    rows = cols // blocks
    seqs = accepted.shape[1]
    tokens = draft * seqs
    width = x_b.shape[1]
    inner = width * n
    bc_here = bc_b.shape[1]
    states = n * bc_here // 2
    kernel = x_w.shape[1]
    dt_row = 2 * width + round_up(bc_here, 16)

    small = [
        pltpu.make_async_copy(out_w.at[1, p.b], ow, load_sem.at[0]),
        pltpu.make_async_copy(out_w.at[0, p.b], whole.at[me, p.b], load_sem.at[1]),
        pltpu.make_async_copy(w_zx, wz, load_sem.at[2]),
        pltpu.make_async_copy(w_bc, wb, load_sem.at[3]),
        pltpu.make_async_copy(ssm, h0, load_sem.at[4]),
    ]
    own = pltpu.make_async_copy(part, stream.at[me], load_sem.at[5])
    own.start()
    for load in small:
        load.start()
    p.greet()

    def w_arrived(e, slot):
        block = whole.at[slot, p.b]
        for k in range(1, nb):
            remote(
                block, block, w_batch.at[0, k, e], w_batch.at[1, k, e], "batch",
                lax.rem(p.b + k, nb),
            ).start()
        remote(block, block, w_mate.at[0, 0, e], w_mate.at[1, 0, e], "heads", p.mate).start()

    w_line_g = Line(p, lambda slot: whole.at[slot, p.b], w_line, w_arrived)

    def line_of(f):
        def arrived(e, slot):
            ref = stream.at[slot, pl.ds(f * rows, rows)]
            remote(
                ref, ref, mate_sems.at[f, 0, e], mate_sems.at[f, 1, e], "heads", p.mate
            ).start()

        return Line(p, lambda slot: stream.at[slot, pl.ds(f * rows, rows)], line_sems.at[f], arrived)

    lines = [line_of(f) for f in range(blocks)]
    own.wait()
    for line in lines:
        line.start()
    small[0].wait()
    own_w = ow[...].astype(F32)
    for d in range(n):
        parts_src[d] = own_w[:, d * cols : (d + 1) * cols].astype(BF16)
    part_g = Spread(
        "heads", me, n, lambda d: parts_src.at[d], lambda d: parts.at[d, p.b], part_sems
    )

    for load in small[2:4]:
        load.wait()
    gcol[...] = jnp.transpose(jnp.concatenate([gain[...], jnp.zeros((6, model), F32)], axis=0))
    for layer in range(LAYERS):
        wl[layer, 0 : 2 * width] = jnp.transpose(wz[layer].astype(F32)).astype(BF16)
        wl[layer, 2 * width :] = jnp.zeros((wl.shape[1] - 2 * width, model), BF16)
        wl[layer, 2 * width : 2 * width + bc_here] = wb[layer]
        wl[layer, dt_row : dt_row + 1] = w_dt[layer : layer + 1, :]
    small[1].wait()
    for d in range(1, p.chips):
        for line in lines:
            line.step(d)
        if d == max(p.chips - 2, 1):
            w_line_g.start()
    for f in range(blocks):
        def landed(e, off, f=f):
            ref = stream.at[p.mate + off, pl.ds(f * rows, rows)]
            remote(
                ref, ref, mate_sems.at[f, 0, e], mate_sems.at[f, 1, e], "heads", p.mate
            ).wait_recv()

        lines[f].each(landed)

    total = jnp.zeros((1, tokens), F32)
    for i in range(n):
        v = stream[i].astype(F32)
        val[i * cols : (i + 1) * cols] = v
        total = total + jnp.sum(v * v, axis=0, keepdims=True)

    row_seq = accepted[...]
    kept = jnp.sum(
        jnp.where(eye(seqs, F32) > 0, jnp.broadcast_to(row_seq, (seqs, seqs)), 0),
        axis=1, keepdims=True,
    )
    row = lax.broadcasted_iota(jnp.int32, (tokens, tokens), 0)
    col = lax.broadcasted_iota(jnp.int32, (tokens, tokens), 1)
    same = (lax.rem(row, seqs) == lax.rem(col, seqs)) & (col <= row)
    diag = row == col

    def at(value, t):
        return value[t * seqs : (t + 1) * seqs]

    def keep_rows(window, j):
        chosen = at(window, 1 + j)
        for a in range(2, draft + 1):
            chosen = jnp.where(kept == a, at(window, a + j), chosen)
        return chosen

    def convolve(window, taps, b):
        acc = window[0:tokens] * taps[0:1].astype(F32)
        for k in range(1, kernel):
            acc = acc + window[k * seqs : k * seqs + tokens] * taps[k : k + 1].astype(F32)
        return silu(acc + b.astype(F32))

    def spread_tokens(ref, value):
        for t in range(draft):
            ref[pl.ds(t, seqs, stride=draft), :] = at(value, t)

    step_rows = model // 8
    for layer in range(LAYERS):
        scale = rms_scale(total, model)
        for i in range(8):
            here = slice(i * step_rows, (i + 1) * step_rows)
            nrm[here] = (val[here] * scale * gcol[here, layer : layer + 1]).astype(BF16)
        zb = dot(wl[layer], nrm[...]).astype(BF16).astype(F32)
        high = round_up(wl.shape[1], LANES)
        zb = jnp.concatenate([zb, jnp.zeros((high - wl.shape[1], tokens), F32)], axis=0)
        tb = jnp.transpose(zb)
        bc = tb[:, 2 * width : 2 * width + bc_here]
        eye_s = eye(seqs, BF16)
        eye_c = eye(bc_here, BF16)
        past = [dot(eye_s, bc_state[layer, j], 1, 1) for j in range(kernel - 1)]
        window_bc = jnp.concatenate(past + [bc], axis=0)
        bcc = convolve(window_bc, bc_w[layer], bc_b[layer : layer + 1])
        bca[layer, me] = dot(eye_c, bcc.astype(BF16), 1, 1).astype(BF16)
        bc_g = Direct(p, bca.at[layer], bc_sems.at[layer])
        bc_g.start()
        if layer == 0:
            w_line_g.step(1)
            part_g.start()
            parts[me, p.b] = parts_src[me]
        for j in range(kernel - 1):
            new_bc[layer, j] = dot(eye_c, keep_rows(window_bc, j).astype(BF16), 1, 1).astype(BF16)
        z = tb[:, :width]
        window_x = jnp.concatenate(
            [x_state[layer, j].astype(F32) for j in range(kernel - 1)] + [tb[:, width : 2 * width]],
            axis=0,
        )
        xc = convolve(window_x, x_w[layer], x_b[layer : layer + 1])
        for j in range(kernel - 1):
            new_x[layer, j] = keep_rows(window_x, j).astype(BF16)
        raw = tb[:, dt_row : dt_row + 1] + bias[0, layer]
        rate, skip = rate_ref[0, layer], skip_ref[0, layer]
        step = jnp.maximum(raw, 0.0) + jnp.log1p(jnp.exp(-jnp.abs(raw)))
        sums = [at(step, 0)]
        for t in range(1, draft):
            sums.append(sums[-1] + at(step, t))
        sum_col = jnp.concatenate(sums, axis=0)
        sum_row = jnp.sum(jnp.where(diag, sum_col, 0.0), axis=0, keepdims=True)
        spread = jnp.exp(jnp.where(same, (sum_row - sum_col) * rate, -1e30))
        xw = xc * step
        final = sums[0]
        for t in range(1, draft):
            final = jnp.where(kept == t + 1, sums[t], final)
        coef = jnp.concatenate(
            [jnp.exp(jnp.where(kept > t, (sums[t] - final) * rate, -1e30)) for t in range(draft)],
            axis=0,
        )
        k_s[...] = jnp.broadcast_to(jnp.exp(-final * rate), k_s.shape)
        spread_tokens(x_s, xw * coef)
        xk_t = jnp.transpose(x_s[...]).astype(BF16)
        if layer == 0:
            small[4].wait()
        bc_g.relay()
        if layer == 0:
            for d in range(2, p.chips):
                w_line_g.step(d)
        bc_g.finish()
        for i in range(n):
            bcf[i * bc_here : (i + 1) * bc_here] = bca[layer, i].astype(F32)
        bcc_all = jnp.transpose(bcf[...])
        b, c = bcc_all[:, :states], bcc_all[:, states:]
        spread_tokens(c_s, c)
        spread_tokens(b_s, b)
        scores = dot(c.astype(BF16), b.astype(BF16), 1, 1) * spread
        y = dot(scores.astype(BF16), xw.astype(BF16))
        for q in range(seqs):
            here = slice(q * draft, (q + 1) * draft)
            y_s[here] = dot(c_s[here].astype(BF16), h0[layer, q].astype(BF16), 1, 1)
        y0 = jnp.concatenate(
            [y_s[pl.ds(t, seqs, stride=draft), :] for t in range(draft)], axis=0
        )
        y = y + jnp.exp(-sum_col * rate) * y0 + skip * xc
        gated = y * silu(z)
        ua[layer, me] = jnp.transpose(gated * gate_gain[layer : layer + 1]).astype(BF16)
        gated_t = jnp.transpose(gated)
        sq[layer, me] = jnp.sum(gated_t * gated_t, axis=0, keepdims=True)
        u_g = Direct(p, ua.at[layer], u_sems.at[layer])
        u_g.start()
        sq_g = Spread(
            "heads", me, n, lambda d: sq.at[layer, me], lambda d: sq.at[layer, d],
            sq_sems.at[layer],
        )
        sq_g.start()
        if layer == 0:
            def cross(e, off):
                for k in range(1, nb):
                    block = whole.at[me + off, lax.rem(p.b + nb - k, nb)]
                    remote(
                        block, block, w_batch.at[0, k, e], w_batch.at[1, k, e], "batch", p.b
                    ).wait_recv()
                    remote(
                        block, block, w_mate.at[0, k, e], w_mate.at[1, k, e], "heads", p.mate
                    ).start()

            w_line_g.each(cross)
            part_g.came()
            part_b = Spread(
                "batch", p.b, nb, lambda d: parts.at[:, p.b], lambda d: parts.at[:, d], part_batch
            )
            part_b.start()
        in_group = LANES // draft
        group_row = lax.broadcasted_iota(jnp.int32, (LANES, states), 0) // draft
        for q in range(seqs):
            g = q // in_group
            mine = jnp.where(
                group_row == q % in_group, b_s[g * LANES : (g + 1) * LANES], 0.0
            )
            added = dot(xk_t[:, g * LANES : (g + 1) * LANES], mine.astype(BF16))
            h1[layer, q] = k_s[q : q + 1] * h0[layer, q] + added
        u_g.relay()
        u_g.finish()
        sq_g.came()
        u_all = ua[layer].reshape(inner, tokens)
        ssq = jnp.sum(sq[layer].reshape(n, tokens), axis=0, keepdims=True)
        out_scale = rms_scale(ssq, inner)
        if layer + 1 < LAYERS:
            def crossed(e, off):
                for k in range(nb):
                    block = whole.at[p.mate + off, lax.rem(p.b + nb - k, nb)]
                    remote(
                        block, block, w_mate.at[0, k, e], w_mate.at[1, k, e], "heads", p.mate
                    ).wait_recv()

            w_line_g.each(crossed)
            total = jnp.zeros((1, tokens), F32)
            lanes = 4 * LANES if model % (4 * LANES) == 0 else LANES
            for ch in range(model // lanes):
                here = slice(ch * lanes, (ch + 1) * lanes)
                w = whole[:, :, :, ch * lanes : (ch + 1) * lanes].reshape(inner, lanes)
                mix = dot(w, u_all, 0, 0) * out_scale
                v = (val[here] + mix).astype(BF16).astype(F32)
                val[here] = v
                total = total + jnp.sum(v * v, axis=0, keepdims=True)
        else:
            part_b.came()
            mix = dot(parts[...].reshape(inner, cols), u_all, 0, 0) * out_scale
            mine = val[pl.ds(pl.multiple_of(me * cols, 8), cols)]
            res = (mine + mix).astype(BF16)
            place = lax.rem(col, draft) * seqs + col // draft
            order = jnp.where(row == place, 1.0, 0.0).astype(BF16)
            hidden[...] = dot(res, order).astype(BF16)
        u_g.sent()
        sq_g.sent()
        bc_g.sent()

    for f in range(blocks):
        lines[f].sent()

        def done(e, off, f=f):
            ref = stream.at[me, pl.ds(f * rows, rows)]
            remote(
                ref, ref, mate_sems.at[f, 0, e], mate_sems.at[f, 1, e], "heads", p.mate
            ).wait_send()

        lines[f].each(done)
    w_line_g.sent()

    def w_done(e, off):
        block = whole.at[me, p.b]
        for k in range(nb):
            remote(
                block, block, w_mate.at[0, k, e], w_mate.at[1, k, e], "heads", p.mate
            ).wait_send()
        for k in range(1, nb):
            remote(
                block, block, w_batch.at[0, k, e], w_batch.at[1, k, e], "batch", p.b
            ).wait_send()

    w_line_g.each(w_done)
    part_g.sent()
    part_b.sent()


def local(
    draft_ids, accepted, embedding, norm_gain, w_zx, w_dt, w_bc, dt_bias, decay_rate,
    skip_weight, conv_x_w, conv_x_b, conv_bc_w, conv_bc_b, gate_gain, out_w, ssm_state,
    conv_x_state, conv_bc_state,
):
    n, nb = lax.axis_size("heads"), lax.axis_size("batch")
    seqs, draft = draft_ids.shape
    tokens = seqs * draft
    width = w_zx.shape[3] // 2
    vocab, cols = embedding.shape
    model = cols * n
    bc_here = w_bc.shape[2]
    states = ssm_state.shape[4]
    kernel = conv_x_w.shape[1]
    share = width // nb
    chips = n // 2
    blocks = 4 if cols % 64 == 0 else 1
    wl_rows = 2 * width + round_up(bc_here, 16) + 16

    part = lookup(draft_ids.T, embedding.T, tokens)
    args = [
        dt_bias.T, decay_rate.T, skip_weight.T, accepted.reshape(1, seqs), norm_gain,
        w_dt.reshape(LAYERS, model), conv_x_w, conv_x_b, conv_bc_w, conv_bc_b, gate_gain,
        conv_x_state.transpose(0, 2, 1, 3), conv_bc_state.transpose(0, 2, 3, 1), part,
        w_zx.reshape(LAYERS, model, 2 * width), w_bc.transpose(0, 2, 1),
        out_w.reshape(LAYERS, nb, share, model), ssm_state.reshape(LAYERS, seqs, width, states),
    ]
    smem = pl.BlockSpec(memory_space=pltpu.SMEM)
    vmem = pl.BlockSpec(memory_space=pltpu.VMEM)
    anywhere = pl.BlockSpec(memory_space=pl.ANY)
    dma = pltpu.SemaphoreType.DMA
    hidden, new_x, new_bc, new_ssm = pl.pallas_call(
        functools.partial(program_kernel, (n, nb, blocks, draft)),
        out_shape=[
            jax.ShapeDtypeStruct((cols, tokens), BF16),
            jax.ShapeDtypeStruct((LAYERS, kernel - 1, seqs, width), BF16),
            jax.ShapeDtypeStruct((LAYERS, kernel - 1, bc_here, seqs), BF16),
            pltpu.VMEM((LAYERS, seqs, width, states), F32),
        ],
        in_specs=[smem] * 3 + [vmem] * 10 + [anywhere] * 5,
        out_specs=[vmem] * 4,
        scratch_shapes=[
            pltpu.VMEM((n, cols, tokens), BF16),
            pltpu.VMEM((model, tokens), F32),
            pltpu.VMEM((model, tokens), BF16),
            pltpu.VMEM((LAYERS, wl_rows, model), BF16),
            pltpu.VMEM((model, 8), F32),
            pltpu.VMEM((LAYERS, model, 2 * width), BF16),
            pltpu.VMEM((LAYERS, bc_here, model), BF16),
            pltpu.VMEM((share, model), BF16),
            pltpu.VMEM((n, share, cols), BF16),
            pltpu.VMEM((n, nb, share, cols), BF16),
            pltpu.VMEM((n, nb, share, model), BF16),
            pltpu.VMEM((LAYERS, n, bc_here, tokens), BF16),
            pltpu.VMEM((n * bc_here, tokens), F32),
            pltpu.VMEM((LAYERS, n, width, tokens), BF16),
            pltpu.VMEM((LAYERS, n, 1, tokens), F32),
            pltpu.VMEM((LAYERS, seqs, width, states), F32),
            pltpu.VMEM((tokens, states), F32),
            pltpu.VMEM((tokens, states), F32),
            pltpu.VMEM((tokens, width), F32),
            pltpu.VMEM((tokens, width), F32),
            pltpu.VMEM((seqs, states), F32),
            dma((6,)),
            dma((blocks, 2, 2, chips)),
            dma((2, 2, chips)),
            dma((2, nb, 2 * chips)),
            dma((2, nb, 2 * chips)),
            dma((blocks, 2, 2 * chips)),
            dma((LAYERS, 2, 2, chips)),
            dma((LAYERS, 2, 2, chips)),
            dma((LAYERS, 2, n)),
            dma((2, n)),
            dma((2, nb)),
        ],
        compiler_params=pltpu.CompilerParams(
            collective_id=0, has_side_effects=True, vmem_limit_bytes=PROGRAM_LIMIT
        ),
        name="program",
    )(*args)
    return (
        hidden.T,
        new_ssm.reshape(ssm_state.shape),
        new_x.transpose(0, 2, 1, 3),
        new_bc.transpose(0, 3, 1, 2),
    )


def solution(mesh):
    placed = (
        P("batch", None),
        P("batch"),
        P(None, "heads"),
        P(),
        P(None, None, "heads", None),
        P(None, None, "heads"),
        P(None, None, "heads"),
        P(None, "heads"),
        P(None, "heads"),
        P(None, "heads"),
        P(None, None, "heads"),
        P(None, "heads"),
        P(None, None, "heads"),
        P(None, "heads"),
        P(None, "heads"),
        P(None, "heads", None),
        P(None, "batch", "heads", None, None),
        P(None, "batch", None, "heads"),
        P(None, "batch", None, "heads"),
    )
    return jax.shard_map(
        local,
        mesh=mesh,
        in_specs=placed,
        out_specs=(
            P("batch", "heads"),
            P(None, "batch", "heads", None, None),
            P(None, "batch", None, "heads"),
            P(None, "batch", None, "heads"),
        ),
        check_vma=False,
    )
```

```python
import functools

import jax
import jax.numpy as jnp
from jax import lax
from jax.experimental import pallas as pl
from jax.experimental.pallas import tpu as pltpu
from jax.sharding import PartitionSpec as P

LAYERS = 2
EPS = 1e-05
MESH = pl.DeviceIdType.MESH
LANES = 128
OUT_LIMIT = 8 * 1024 * 1024
PROGRAM_LIMIT = 58 * 1024 * 1024
F32, BF16 = jnp.float32, jnp.bfloat16


def rms_scale(total, count):
    return lax.rsqrt(total / count + EPS)


def dot(a, b, ca=1, cb=0):
    return lax.dot_general(a, b, (((ca,), (cb,)), ((), ())), preferred_element_type=F32)


def round_up(x, m):
    return -(-x // m) * m


def silu(v):
    return v * (1.0 / (1.0 + jnp.exp(-v)))


def eye(n, dtype):
    row = lax.broadcasted_iota(jnp.int32, (n, n), 0)
    col = lax.broadcasted_iota(jnp.int32, (n, n), 1)
    return jnp.where(row == col, 1.0, 0.0).astype(dtype)


def remote(src, dst, send, recv, axis, device):
    return pltpu.make_async_remote_copy(
        src_ref=src, dst_ref=dst, send_sem=send, recv_sem=recv,
        device_id={axis: device}, device_id_type=MESH,
    )


class Place:
    def __init__(self, n, nb):
        self.n, self.nb, self.chips = n, nb, n // 2
        self.me = lax.axis_index("heads")
        self.b = lax.axis_index("batch")
        self.core = lax.rem(self.me, 2)
        self.chip = self.me // 2
        self.mate = self.me + 1 - 2 * self.core
        self.last = self.chips - 1

    def greet(self):
        barrier = pltpu.get_barrier_semaphore()
        for d in range(1, self.n):
            pl.semaphore_signal(
                barrier, inc=1, device_id={"heads": lax.rem(self.me + d, self.n)},
                device_id_type=MESH,
            )
        for k in range(1, self.nb):
            pl.semaphore_signal(
                barrier, inc=1, device_id={"batch": lax.rem(self.b + k, self.nb)},
                device_id_type=MESH,
            )

    def greeted(self):
        pl.semaphore_wait(pltpu.get_barrier_semaphore(), self.n + self.nb - 2)


class Line:
    def __init__(self, place, buf, sems, arrived):
        self.p, self.buf, self.sems, self.arrived = place, buf, sems, arrived

    def copy(self, kind, d, slot, device):
        ref = self.buf(slot)
        return remote(ref, ref, self.sems.at[kind, 0, d], self.sems.at[kind, 1, d], "heads", device)

    def start(self):
        p = self.p

        @pl.when(p.chip < p.last)
        def _():
            self.copy(0, 0, p.me, p.me + 2).start()

        @pl.when(p.chip > 0)
        def _():
            self.copy(1, 0, p.me, p.me - 2).start()

        self.arrived(0, p.me)

    def step(self, d):
        p = self.p

        @pl.when(p.chip >= d)
        def _():
            slot = p.me - 2 * d
            self.copy(0, d - 1, slot, slot).wait_recv()

            @pl.when(p.chip < p.last)
            def _():
                self.copy(0, d, slot, p.me + 2).start()

            self.arrived(d, slot)

        @pl.when(p.chip + d <= p.last)
        def _():
            slot = p.me + 2 * d
            self.copy(1, d - 1, slot, slot).wait_recv()

            @pl.when(p.chip > 0)
            def _():
                self.copy(1, d, slot, p.me - 2).start()

            self.arrived(p.last + d, slot)

    def each(self, fn):
        p = self.p
        fn(0, 0)
        for d in range(1, p.chips):
            @pl.when(p.chip >= d)
            def _(d=d):
                fn(d, -2 * d)

            @pl.when(p.chip + d <= p.last)
            def _(d=d):
                fn(p.last + d, 2 * d)

    def sent(self):
        p = self.p
        for d in range(p.chips - 1):
            @pl.when((p.chip >= d) & (p.chip < p.last))
            def _(d=d):
                self.copy(0, d, p.me, p.me).wait_send()

            @pl.when((p.chip + d <= p.last) & (p.chip > 0))
            def _(d=d):
                self.copy(1, d, p.me, p.me).wait_send()


class Direct:
    def __init__(self, place, out, sems):
        self.p, self.out, self.sems = place, out, sems

    def copy(self, slot, device, kind, e):
        ref = self.out.at[slot]
        return remote(ref, ref, self.sems.at[kind, 0, e], self.sems.at[kind, 1, e], "heads", device)

    def peers(self, distances, fn):
        p = self.p
        for d in distances:
            @pl.when(p.chip + d <= p.last)
            def _(d=d):
                fn(d, 2 * d)

            @pl.when(p.chip >= d)
            def _(d=d):
                fn(p.last + d, -2 * d)

    def start(self):
        p = self.p
        self.copy(p.me, p.mate, 0, 0).start()
        self.peers(
            range(p.last, 0, -1), lambda e, off: self.copy(p.me, p.me + off, 0, e).start()
        )

    def other(self, e):
        last = self.p.last
        return e + last if e <= last else e - last

    def relay(self):
        p = self.p

        def pass_on(e, off):
            self.copy(p.me + off, p.me, 0, self.other(e)).wait_recv()
            self.copy(p.me + off, p.mate, 1, e).start()

        self.peers(range(1, p.chips), pass_on)

    def finish(self):
        p = self.p
        self.copy(p.mate, p.mate, 0, 0).wait_recv()
        self.peers(
            range(1, p.chips), lambda e, off: self.copy(p.mate + off, p.mate, 1, e).wait_recv()
        )

    def sent(self):
        p = self.p
        self.copy(p.me, p.mate, 0, 0).wait_send()

        def gone(e, off):
            self.copy(p.me, p.mate, 0, e).wait_send()
            self.copy(p.me, p.mate, 1, e).wait_send()

        self.peers(range(1, p.chips), gone)


class Spread:
    def __init__(self, axis, me, n, src, dst, sems):
        self.axis, self.me, self.n = axis, me, n
        self.src, self.dst, self.sems = src, dst, sems

    def copy(self, d, peer, at):
        return remote(
            self.src(peer), self.dst(at), self.sems.at[0, d], self.sems.at[1, d], self.axis, peer
        )

    def start(self):
        for d in range(1, self.n):
            self.copy(d, lax.rem(self.me + d, self.n), self.me).start()

    def came(self):
        for d in range(1, self.n):
            peer = lax.rem(self.me + self.n - d, self.n)
            self.copy(d, peer, peer).wait_recv()

    def sent(self):
        for d in range(1, self.n):
            self.copy(d, lax.rem(self.me + d, self.n), self.me).wait_send()


class Lookup:
    def __init__(self, ids, tail, table, tabs, pick, tiles, sems, rows):
        self.ids, self.tail, self.table, self.tabs = ids, tail, table, tabs
        self.pick, self.tiles, self.sems, self.rows = pick, tiles, sems, rows
        self.full = table.shape[1] // LANES

    def tab(self, f):
        return self.tabs[f % len(self.tabs)]

    def load(self, f):
        here = pl.ds(f * self.rows, self.rows)

        def one(i, carry):
            pltpu.make_async_copy(
                self.table.at[here, pl.ds(pl.multiple_of(i * LANES, LANES), LANES)],
                self.tab(f).at[i], self.sems.at[f],
            ).start()
            return carry

        lax.fori_loop(0, self.full, one, 0, unroll=8 if self.full % 8 == 0 else 1)

    def build(self, at, place):
        seqs = self.ids.shape[1]
        token = self.ids[at // seqs, lax.rem(at, seqs)]
        row = lax.broadcasted_iota(jnp.int32, (LANES, LANES), 0)
        col = lax.broadcasted_iota(jnp.int32, (LANES, LANES), 1)
        self.tiles[at] = token >> 7
        one = (row == (token & (LANES - 1))) & (col == (at & (LANES - 1)))
        here = pl.ds(pl.multiple_of(place * LANES, LANES), LANES)
        self.pick[here, :] = jnp.where(one, 1.0, 0.0).astype(BF16)

    def prepare(self):
        if self.pick.shape[0] == LANES * LANES:
            return
        draft, seqs = self.ids.shape
        row = lax.broadcasted_iota(jnp.int32, (LANES, LANES), 0)
        col = lax.broadcasted_iota(jnp.int32, (LANES, LANES), 1)
        for t in range(draft):
            def build(s, carry, t=t):
                at = t * seqs + s
                token = self.ids[t, s]
                self.tiles[at] = token >> 7
                one = (row == (token & (LANES - 1))) & (col == (at & (LANES - 1)))
                here = pl.ds(pl.multiple_of(at * LANES, LANES), LANES)
                self.pick[here, :] = jnp.where(one, 1.0, 0.0).astype(BF16)
                return carry

            lax.fori_loop(0, seqs, build, 0, unroll=8 if seqs % 8 == 0 else 1)

    def take(self, f, put):
        tab = self.tab(f)
        whole = tab.at[pl.ds(0, self.full)]
        pltpu.make_async_copy(whole, whole, self.sems.at[f]).wait()
        tab[self.full] = self.tail[f * self.rows : (f + 1) * self.rows]

        grouped = self.pick.shape[0] == LANES * LANES

        def group(g, carry):
            if grouped:
                def build(k, inner):
                    self.build(g * LANES + k, k)
                    return inner

                lax.fori_loop(0, LANES, build, 0)
            found = jnp.concatenate(
                [tab[self.tiles[g * LANES + k]] for k in range(LANES)], axis=1
            )
            first = 0 if grouped else pl.multiple_of(g * LANES * LANES, LANES)
            here = pl.ds(first, LANES * LANES)
            put(g, dot(found, self.pick[here, :]).astype(BF16))
            return carry

        draft, seqs = self.ids.shape
        lax.fori_loop(0, draft * seqs // LANES, group, 0)


def out_kernel(*refs):
    count = len(refs) // 2
    sems = refs[-1]
    copies = [
        pltpu.make_async_copy(refs[i], refs[count + i], sems.at[i]) for i in range(count)
    ]
    for copy in copies:
        copy.start()
    for copy in copies:
        copy.wait()


def put_out(arrays):
    count = len(arrays)
    return pl.pallas_call(
        out_kernel,
        out_shape=[jax.ShapeDtypeStruct(a.shape, a.dtype) for a in arrays],
        in_specs=[pl.BlockSpec(memory_space=pltpu.VMEM)] * count,
        out_specs=[pl.BlockSpec(memory_space=pl.ANY)] * count,
        scratch_shapes=[pltpu.SemaphoreType.DMA((count,))],
        compiler_params=pltpu.CompilerParams(vmem_limit_bytes=OUT_LIMIT),
        name="put_out",
    )(*arrays)


def program_kernel(cfg, *refs):
    n, nb, blocks = cfg
    (ids, tail, table, bias, rate_ref, skip_ref, accepted, gain, w_dt, x_w, x_b, bc_w, bc_b, gate_gain,
     x_state, bc_state, w_zx, w_bc, out_w, ssm,
     hidden, new_x, new_bc, h1) = refs[:24]
    slots = min(blocks, 3)
    tabs, refs = refs[24 : 24 + slots], refs[24 + slots :]
    (pick, tiles, table_sem, stream, val, nrm, wl, gcol, wz, wb, ow, parts_src, parts, whole, bca, bcf, ua, sq,
     c_s, b_s, x_s, y_s, k_s,
     load_sem, line_sems, w_line, w_batch, w_mate,
     mate_sems, bc_sems, u_sems, sq_sems, part_sems, part_batch) = refs
    p = Place(n, nb)
    me = p.me
    cols = table.shape[0]
    model = cols * n
    rows = cols // blocks
    draft, seqs = ids.shape
    tokens = draft * seqs
    width = x_b.shape[1]
    inner = width * n
    bc_here = bc_b.shape[1]
    states = n * bc_here // 2
    kernel = x_w.shape[1]
    dt_row = 2 * width + round_up(bc_here, 16)

    small = [
        pltpu.make_async_copy(out_w.at[1, p.b], ow, load_sem.at[0]),
        pltpu.make_async_copy(out_w.at[0, p.b], whole.at[me, p.b], load_sem.at[1]),
        pltpu.make_async_copy(w_zx, wz, load_sem.at[2]),
        pltpu.make_async_copy(w_bc, wb, load_sem.at[3]),
        pltpu.make_async_copy(ssm, h1, load_sem.at[4]),
    ]
    find = Lookup(ids, tail, table, tabs, pick, tiles, table_sem, rows)
    p.greet()
    for load in small[:2]:
        load.start()
    ahead = min(slots, 2)
    for f in range(ahead):
        find.load(f)
    for load in small[2:]:
        load.start()
    p.greeted()

    def w_arrived(e, slot):
        block = whole.at[slot, p.b]
        for k in range(1, nb):
            remote(
                block, block, w_batch.at[0, k, e], w_batch.at[1, k, e], "batch",
                lax.rem(p.b + k, nb),
            ).start()
        remote(block, block, w_mate.at[0, 0, e], w_mate.at[1, 0, e], "heads", p.mate).start()

    w_line_g = Line(p, lambda slot: whole.at[slot, p.b], w_line, w_arrived)

    def line_of(f):
        def arrived(e, slot):
            ref = stream.at[slot, pl.ds(f * rows, rows)]
            remote(
                ref, ref, mate_sems.at[f, 0, e], mate_sems.at[f, 1, e], "heads", p.mate
            ).start()

        return Line(p, lambda slot: stream.at[slot, pl.ds(f * rows, rows)], line_sems.at[f], arrived)

    lines = [line_of(f) for f in range(blocks)]
    small[1].wait()
    w_line_g.start()
    find.prepare()
    small[0].wait()
    own_w = ow[...].astype(F32)
    for d in range(n):
        parts_src[d] = own_w[:, d * cols : (d + 1) * cols].astype(BF16)
    part_g = Spread(
        "heads", me, n, lambda d: parts_src.at[d], lambda d: parts.at[d, p.b], part_sems
    )

    for wave in range(blocks + p.chips - 1):
        if wave < blocks:
            def put(g, block, f=wave):
                at = pl.ds(pl.multiple_of(g * LANES, LANES), LANES)
                stream[me, pl.ds(f * rows, rows), at] = block

            find.take(wave, put)
            lines[wave].start()
            if wave + ahead < blocks:
                find.load(wave + ahead)
        for f in range(blocks):
            d = wave - f
            if 1 <= d < p.chips:
                lines[f].step(d)
        if 1 <= wave < p.last:
            w_line_g.step(wave)
        if wave == blocks - 1:
            for load in small[2:4]:
                load.wait()
            gcol[...] = jnp.transpose(jnp.concatenate([gain[...], jnp.zeros((6, model), F32)], axis=0))
            for layer in range(LAYERS):
                wl[layer, 0 : 2 * width] = jnp.transpose(wz[layer].astype(F32)).astype(BF16)
                wl[layer, 2 * width :] = jnp.zeros((wl.shape[1] - 2 * width, model), BF16)
                wl[layer, 2 * width : 2 * width + bc_here] = wb[layer]
                wl[layer, dt_row : dt_row + 1] = w_dt[layer : layer + 1, :]
    for f in range(blocks):
        def landed(e, off, f=f):
            ref = stream.at[p.mate + off, pl.ds(f * rows, rows)]
            remote(
                ref, ref, mate_sems.at[f, 0, e], mate_sems.at[f, 1, e], "heads", p.mate
            ).wait_recv()

        lines[f].each(landed)

    total = jnp.zeros((1, tokens), F32)
    for i in range(n):
        v = stream[i].astype(F32)
        val[i * cols : (i + 1) * cols] = v
        total = total + jnp.sum(v * v, axis=0, keepdims=True)

    row_seq = accepted[...]
    kept = jnp.sum(
        jnp.where(eye(seqs, F32) > 0, jnp.broadcast_to(row_seq, (seqs, seqs)), 0),
        axis=1, keepdims=True,
    )
    row = lax.broadcasted_iota(jnp.int32, (tokens, tokens), 0)
    col = lax.broadcasted_iota(jnp.int32, (tokens, tokens), 1)
    same = (lax.rem(row, seqs) == lax.rem(col, seqs)) & (col <= row)
    diag = row == col

    def at(value, t):
        return value[t * seqs : (t + 1) * seqs]

    def keep_rows(window, j):
        chosen = at(window, 1 + j)
        for a in range(2, draft + 1):
            chosen = jnp.where(kept == a, at(window, a + j), chosen)
        return chosen

    def convolve(window, taps, b):
        acc = window[0:tokens] * taps[0:1].astype(F32)
        for k in range(1, kernel):
            acc = acc + window[k * seqs : k * seqs + tokens] * taps[k : k + 1].astype(F32)
        return silu(acc + b.astype(F32))

    def spread_tokens(ref, value):
        for t in range(draft):
            ref[pl.ds(t, seqs, stride=draft), :] = at(value, t)

    step_rows = model // 8
    for layer in range(LAYERS):
        scale = rms_scale(total, model)
        for i in range(8):
            here = slice(i * step_rows, (i + 1) * step_rows)
            nrm[here] = (val[here] * scale * gcol[here, layer : layer + 1]).astype(BF16)
        zb = dot(wl[layer], nrm[...]).astype(BF16).astype(F32)
        high = round_up(wl.shape[1], LANES)
        zb = jnp.concatenate([zb, jnp.zeros((high - wl.shape[1], tokens), F32)], axis=0)
        tb = jnp.transpose(zb)
        bc = tb[:, 2 * width : 2 * width + bc_here]
        eye_s = eye(seqs, BF16)
        eye_c = eye(bc_here, BF16)
        past = [dot(eye_s, bc_state[layer, j], 1, 1) for j in range(kernel - 1)]
        window_bc = jnp.concatenate(past + [bc], axis=0)
        bcc = convolve(window_bc, bc_w[layer], bc_b[layer : layer + 1])
        bca[layer, me] = dot(eye_c, bcc.astype(BF16), 1, 1).astype(BF16)
        bc_g = Direct(p, bca.at[layer], bc_sems.at[layer])
        bc_g.start()
        if layer == 0:
            part_g.start()
            parts[me, p.b] = parts_src[me]
        for j in range(kernel - 1):
            new_bc[layer, j] = dot(eye_c, keep_rows(window_bc, j).astype(BF16), 1, 1).astype(BF16)
        z = tb[:, :width]
        window_x = jnp.concatenate(
            [x_state[layer, j].astype(F32) for j in range(kernel - 1)] + [tb[:, width : 2 * width]],
            axis=0,
        )
        xc = convolve(window_x, x_w[layer], x_b[layer : layer + 1])
        for j in range(kernel - 1):
            new_x[layer, j] = keep_rows(window_x, j).astype(BF16)
        raw = tb[:, dt_row : dt_row + 1] + bias[0, layer]
        rate, skip = rate_ref[0, layer], skip_ref[0, layer]
        step = jnp.maximum(raw, 0.0) + jnp.log1p(jnp.exp(-jnp.abs(raw)))
        sums = [at(step, 0)]
        for t in range(1, draft):
            sums.append(sums[-1] + at(step, t))
        sum_col = jnp.concatenate(sums, axis=0)
        sum_row = jnp.sum(jnp.where(diag, sum_col, 0.0), axis=0, keepdims=True)
        spread = jnp.exp(jnp.where(same, (sum_row - sum_col) * rate, -1e30))
        xw = xc * step
        final = sums[0]
        for t in range(1, draft):
            final = jnp.where(kept == t + 1, sums[t], final)
        coef = jnp.concatenate(
            [jnp.exp(jnp.where(kept > t, (sums[t] - final) * rate, -1e30)) for t in range(draft)],
            axis=0,
        )
        k_s[...] = jnp.broadcast_to(jnp.exp(-final * rate), k_s.shape)
        spread_tokens(x_s, xw * coef)
        xk_t = jnp.transpose(x_s[...]).astype(BF16)
        if layer == 0:
            small[4].wait()
        bc_g.relay()
        if layer == 0:
            w_line_g.step(p.last)
        bc_g.finish()
        for i in range(n):
            bcf[i * bc_here : (i + 1) * bc_here] = bca[layer, i].astype(F32)
        bcc_all = jnp.transpose(bcf[...])
        b, c = bcc_all[:, :states], bcc_all[:, states:]
        spread_tokens(c_s, c)
        spread_tokens(b_s, b)
        scores = dot(c.astype(BF16), b.astype(BF16), 1, 1) * spread
        y = dot(scores.astype(BF16), xw.astype(BF16))
        for q in range(seqs):
            here = slice(q * draft, (q + 1) * draft)
            y_s[here] = dot(c_s[here].astype(BF16), h1[layer, q].astype(BF16), 1, 1)
        y0 = jnp.concatenate(
            [y_s[pl.ds(t, seqs, stride=draft), :] for t in range(draft)], axis=0
        )
        y = y + jnp.exp(-sum_col * rate) * y0 + skip * xc
        gated = y * silu(z)
        ua[layer, me] = jnp.transpose(gated * gate_gain[layer : layer + 1]).astype(BF16)
        gated_t = jnp.transpose(gated)
        sq[layer, me] = jnp.sum(gated_t * gated_t, axis=0, keepdims=True)
        u_g = Direct(p, ua.at[layer], u_sems.at[layer])
        u_g.start()
        sq_g = Spread(
            "heads", me, n, lambda d: sq.at[layer, me], lambda d: sq.at[layer, d],
            sq_sems.at[layer],
        )
        sq_g.start()
        if layer == 0:
            def cross(e, off):
                for k in range(1, nb):
                    block = whole.at[me + off, lax.rem(p.b + nb - k, nb)]
                    remote(
                        block, block, w_batch.at[0, k, e], w_batch.at[1, k, e], "batch", p.b
                    ).wait_recv()
                    remote(
                        block, block, w_mate.at[0, k, e], w_mate.at[1, k, e], "heads", p.mate
                    ).start()

            w_line_g.each(cross)
            part_g.came()
            part_b = Spread(
                "batch", p.b, nb, lambda d: parts.at[:, p.b], lambda d: parts.at[:, d], part_batch
            )
            part_b.start()
        in_group = LANES // draft
        group_row = lax.broadcasted_iota(jnp.int32, (LANES, states), 0) // draft
        for q in range(seqs):
            g = q // in_group
            mine = jnp.where(
                group_row == q % in_group, b_s[g * LANES : (g + 1) * LANES], 0.0
            )
            added = dot(xk_t[:, g * LANES : (g + 1) * LANES], mine.astype(BF16))
            h1[layer, q] = k_s[q : q + 1] * h1[layer, q] + added
        u_g.relay()
        u_g.finish()
        sq_g.came()
        u_all = ua[layer].reshape(inner, tokens)
        ssq = jnp.sum(sq[layer].reshape(n, tokens), axis=0, keepdims=True)
        out_scale = rms_scale(ssq, inner)
        if layer + 1 < LAYERS:
            def crossed(e, off):
                for k in range(nb):
                    block = whole.at[p.mate + off, lax.rem(p.b + nb - k, nb)]
                    remote(
                        block, block, w_mate.at[0, k, e], w_mate.at[1, k, e], "heads", p.mate
                    ).wait_recv()

            w_line_g.each(crossed)
            total = jnp.zeros((1, tokens), F32)
            lanes = 4 * LANES if model % (4 * LANES) == 0 else LANES
            for ch in range(model // lanes):
                here = slice(ch * lanes, (ch + 1) * lanes)
                w = whole[:, :, :, ch * lanes : (ch + 1) * lanes].reshape(inner, lanes)
                mix = dot(w, u_all, 0, 0) * out_scale
                v = (val[here] + mix).astype(BF16).astype(F32)
                val[here] = v
                total = total + jnp.sum(v * v, axis=0, keepdims=True)
        else:
            part_b.came()
            mix = dot(parts[...].reshape(inner, cols), u_all, 0, 0) * out_scale
            mine = val[pl.ds(pl.multiple_of(me * cols, 8), cols)]
            res = (mine + mix).astype(BF16)
            place = lax.rem(col, draft) * seqs + col // draft
            order = jnp.where(row == place, 1.0, 0.0).astype(BF16)
            hidden[...] = dot(res, order).astype(BF16)
        u_g.sent()
        sq_g.sent()
        bc_g.sent()

    for f in range(blocks):
        lines[f].sent()

        def done(e, off, f=f):
            ref = stream.at[me, pl.ds(f * rows, rows)]
            remote(
                ref, ref, mate_sems.at[f, 0, e], mate_sems.at[f, 1, e], "heads", p.mate
            ).wait_send()

        lines[f].each(done)
    w_line_g.sent()

    def w_done(e, off):
        block = whole.at[me, p.b]
        for k in range(nb):
            remote(
                block, block, w_mate.at[0, k, e], w_mate.at[1, k, e], "heads", p.mate
            ).wait_send()
        for k in range(1, nb):
            remote(
                block, block, w_batch.at[0, k, e], w_batch.at[1, k, e], "batch", p.b
            ).wait_send()

    w_line_g.each(w_done)
    part_g.sent()
    part_b.sent()


def local(
    draft_ids, accepted, embedding, norm_gain, w_zx, w_dt, w_bc, dt_bias, decay_rate,
    skip_weight, conv_x_w, conv_x_b, conv_bc_w, conv_bc_b, gate_gain, out_w, ssm_state,
    conv_x_state, conv_bc_state,
):
    n, nb = lax.axis_size("heads"), lax.axis_size("batch")
    seqs, draft = draft_ids.shape
    tokens = seqs * draft
    width = w_zx.shape[3] // 2
    vocab, cols = embedding.shape
    model = cols * n
    bc_here = w_bc.shape[2]
    states = ssm_state.shape[4]
    kernel = conv_x_w.shape[1]
    share = width // nb
    chips = n // 2
    blocks = 4 if cols % 64 == 0 else 1
    wl_rows = 2 * width + round_up(bc_here, 16) + 16

    table = embedding.T
    vocab = table.shape[1]
    full = vocab // LANES
    slots = min(blocks, 3)
    args = [
        draft_ids.T, table, table, dt_bias.T, decay_rate.T, skip_weight.T, accepted.reshape(1, seqs), norm_gain,
        w_dt.reshape(LAYERS, model), conv_x_w, conv_x_b, conv_bc_w, conv_bc_b, gate_gain,
        conv_x_state.transpose(0, 2, 1, 3), conv_bc_state.transpose(0, 2, 3, 1),
        w_zx.reshape(LAYERS, model, 2 * width), w_bc.transpose(0, 2, 1),
        out_w.reshape(LAYERS, nb, share, model), ssm_state.reshape(LAYERS, seqs, width, states),
    ]
    smem = pl.BlockSpec(memory_space=pltpu.SMEM)
    vmem = pl.BlockSpec(memory_space=pltpu.VMEM)
    anywhere = pl.BlockSpec(memory_space=pl.ANY)
    dma = pltpu.SemaphoreType.DMA
    results = pl.pallas_call(
        functools.partial(program_kernel, (n, nb, blocks)),
        grid=(1,),
        out_shape=[
            pltpu.VMEM((cols, tokens), BF16),
            pltpu.VMEM((LAYERS, kernel - 1, seqs, width), BF16),
            pltpu.VMEM((LAYERS, kernel - 1, bc_here, seqs), BF16),
            pltpu.VMEM((LAYERS, seqs, width, states), F32),
        ],
        in_specs=[smem, pl.BlockSpec((cols, LANES), lambda i: (0, full)), anywhere]
        + [smem] * 3 + [vmem] * 10 + [anywhere] * 4,
        out_specs=[vmem] * 4,
        scratch_shapes=[pltpu.VMEM((full + 1, cols // blocks, LANES), BF16)] * slots
        + [
            pltpu.VMEM(((tokens if blocks > 1 else LANES) * LANES, LANES), BF16),
            pltpu.SMEM((tokens,), jnp.int32),
            dma((blocks,)),
            pltpu.VMEM((n, cols, tokens), BF16),
            pltpu.VMEM((model, tokens), F32),
            pltpu.VMEM((model, tokens), BF16),
            pltpu.VMEM((LAYERS, wl_rows, model), BF16),
            pltpu.VMEM((model, 8), F32),
            pltpu.VMEM((LAYERS, model, 2 * width), BF16),
            pltpu.VMEM((LAYERS, bc_here, model), BF16),
            pltpu.VMEM((share, model), BF16),
            pltpu.VMEM((n, share, cols), BF16),
            pltpu.VMEM((n, nb, share, cols), BF16),
            pltpu.VMEM((n, nb, share, model), BF16),
            pltpu.VMEM((LAYERS, n, bc_here, tokens), BF16),
            pltpu.VMEM((n * bc_here, tokens), F32),
            pltpu.VMEM((LAYERS, n, width, tokens), BF16),
            pltpu.VMEM((LAYERS, n, 1, tokens), F32),
            pltpu.VMEM((tokens, states), F32),
            pltpu.VMEM((tokens, states), F32),
            pltpu.VMEM((tokens, width), F32),
            pltpu.VMEM((tokens, width), F32),
            pltpu.VMEM((seqs, states), F32),
            dma((6,)),
            dma((blocks, 2, 2, chips)),
            dma((2, 2, chips)),
            dma((2, nb, 2 * chips)),
            dma((2, nb, 2 * chips)),
            dma((blocks, 2, 2 * chips)),
            dma((LAYERS, 2, 2, 2 * chips)),
            dma((LAYERS, 2, 2, 2 * chips)),
            dma((LAYERS, 2, n)),
            dma((2, n)),
            dma((2, nb)),
        ],
        compiler_params=pltpu.CompilerParams(
            collective_id=0, has_side_effects=True, vmem_limit_bytes=PROGRAM_LIMIT
        ),
        name="program",
    )(*args)
    hidden, new_x, new_bc, new_ssm = put_out(results)
    return (
        hidden.T,
        new_ssm.reshape(ssm_state.shape),
        new_x.transpose(0, 2, 1, 3),
        new_bc.transpose(0, 3, 1, 2),
    )


def solution(mesh):
    placed = (
        P("batch", None),
        P("batch"),
        P(None, "heads"),
        P(),
        P(None, None, "heads", None),
        P(None, None, "heads"),
        P(None, None, "heads"),
        P(None, "heads"),
        P(None, "heads"),
        P(None, "heads"),
        P(None, None, "heads"),
        P(None, "heads"),
        P(None, None, "heads"),
        P(None, "heads"),
        P(None, "heads"),
        P(None, "heads", None),
        P(None, "batch", "heads", None, None),
        P(None, "batch", None, "heads"),
        P(None, "batch", None, "heads"),
    )
    return jax.shard_map(
        local,
        mesh=mesh,
        in_specs=placed,
        out_specs=(
            P("batch", "heads"),
            P(None, "batch", "heads", None, None),
            P(None, "batch", None, "heads"),
            P(None, "batch", None, "heads"),
        ),
        check_vma=False,
    )
```
